256 devices in a mesh: blk: 8 (over x, core), grp: 32 (over z, y).
Axes of the slice: x: 4, y: 4, z: 8, core: 2. Of those that a mesh axis runs over, the one named last changes fastest.
Arguments:
- features: float32 [393216, 256], P(('blk', 'grp')), may hold values from -6 to 6
- initial: bfloat16 [393216, 256], P(('blk', 'grp')), may hold values from -6 to 6
- history: bfloat16 [393216, 256], P(('blk', 'grp')), may hold values from -6 to 6
- weight: bfloat16 [256, 256], replicated, may hold values from -0.375 to 0.375
- column_ids: int32 [3072, 16], P(('blk', 'grp')), may hold values from 0 to 51, as said below
- block_values: bfloat16 [3072, 16, 128, 128], P(('blk', 'grp')), may hold values from -0.125 to 0.125
- group_table: int32 [8, 32, 32], P('blk'), may hold values from 0 to 11
- loop_table: int32 [32, 8, 8], P('grp'), may hold values from 0 to 11
Outputs:
- refreshed: float32 [393216, 256], P(('blk', 'grp'))
- inbox: float32 [393216, 256], P(('blk', 'grp'))
The draws below stay inside these ranges and needn't reach their ends.
Inputs may be any that keep to these rules, and one draw needn't show every extreme that they name: `column_ids`: among the 16 entries of the 12 row tiles of one device, every slot from 0 to 12 + 32 + 8 - 1 appears at least once.
All inputs are finite; a program needn't handle non-finite values.
Results may differ from the reference program's by a relative error of at most 0.004.
Values may be sent and summed in bfloat16 or wider, within the bound.
No kernel may reach another device: no remote copies, remote signals or barrier semaphores. Data moves between devices by JAX's collectives and lax.ppermute only.
A program may use at most 128 MiB of HBM per device.

```python
import math
import jax
import jax.numpy as jnp
import numpy as np
from jax import lax

H = 256
TILE = 128
K = 16
BLK_DEV = 12
TILES = 3072
NODES = 393216
N_BLK = 8
N_GRP = 32


def draw_column_ids(key, part):
    slots = BLK_DEV + N_GRP + N_BLK
    count = BLK_DEV * K
    device_count = N_BLK * N_GRP
    device_keys = jax.random.split(jax.random.fold_in(key, 7), device_count)

    def one_device(device_key):
        first_key, second_key = jax.random.split(device_key)
        extra = jax.random.randint(first_key, (count - slots,), 0, slots).astype(jnp.int32)
        base = jnp.concatenate([jnp.arange(slots, dtype=jnp.int32), extra])
        return jax.random.permutation(second_key, base).reshape(BLK_DEV, K)
    return jax.vmap(one_device)(device_keys).reshape(device_count * BLK_DEV, K).astype(jnp.int32)


def plant(result, stream_key, least, high):
    spot = [jax.random.randint(jax.random.fold_in(stream_key, axis), (), 0, length) for axis, length in enumerate(result.shape)]
    main_axis = result.shape.index(max(result.shape))
    next_to = spot[:main_axis] + [(spot[main_axis] + 1) % result.shape[main_axis]] + spot[main_axis + 1:]
    return result.at[tuple(spot)].set(least).at[tuple(next_to)].set(high)


def steps_of(own_key, dims, pieces, low, high):
    gain, own = 1.0, jax.random.fold_in(own_key, 6)
    for dim, shards_of in pieces:
        draws = jnp.exp(jax.random.uniform(jax.random.fold_in(own, dim), (shards_of,), jnp.float32, low / len(pieces), high / len(pieces)))
        gain = gain * jnp.repeat(draws, dims[dim] // shards_of).reshape([-1 if axis == dim else 1 for axis in range(len(dims))])
    return gain


def cumulative_ranks(number_of, skew):
    portions = [(1 << 20) // math.isqrt(rank ** skew) + 1 for rank in range(1, number_of + 1)]
    scale = 1 + sum(portions) // (1 << 30)
    return np.cumsum(np.array([max(1, weight // scale) for weight in portions]))


def skewed_ids(stream_key, extent, number_of, slope):
    grid = cumulative_ranks(number_of, slope)
    pick = jax.random.randint(jax.random.fold_in(stream_key, 1), extent, 0, int(grid[number_of - 1]))
    rank = jnp.searchsorted(jnp.asarray(grid, jnp.int32), pick, side="right")
    return jax.random.permutation(jax.random.fold_in(stream_key, 2), number_of)[rank].astype(jnp.int32)


def centred(key, shape, spread, limit, shards=(), kind=jnp.bfloat16):
    array = spread * jax.random.normal(key, shape, jnp.float32)
    if shards:
        array = array * steps_of(key, shape, shards, -0.22, 0.18)
    return jnp.clip(array, -limit, limit).astype(kind)


def setup_inputs(seed: int = 0) -> dict:
    seeds = jax.random.split(jax.random.key(seed), 9)
    features = centred(seeds[0], (NODES, H), 1.0, 6.0, ((0, 256),), jnp.float32)
    initial = centred(seeds[1], (NODES, H), 1.0, 6.0, ((0, 256),))
    history = centred(seeds[2], (NODES, H), 1.0, 6.0, ((0, 256),))
    weight = centred(seeds[3], (H, H), H ** -0.5, 0.375)
    column_ids = draw_column_ids(jax.random.fold_in(seeds[8], 71), 0)
    block_values = centred(seeds[5], (TILES, K, TILE, TILE), (TILE * K) ** -0.5, 0.125, ((0, 256),))
    group_table = plant(skewed_ids(seeds[6], (N_BLK, N_GRP, N_GRP), BLK_DEV, 2), jax.random.fold_in(seeds[6], 3), 0, BLK_DEV - 1).astype(jnp.int32)
    loop_table = plant(skewed_ids(seeds[7], (N_GRP, N_BLK, N_BLK), BLK_DEV, 2), jax.random.fold_in(seeds[7], 3), 0, BLK_DEV - 1).astype(jnp.int32)
    return {"features": features, "initial": initial, "history": history, "weight": weight, "column_ids": column_ids, "block_values": block_values, "group_table": group_table, "loop_table": loop_table}


teleport = 0.1
mapping_share = 0.5


def reference(features, initial, history, weight, column_ids, block_values, group_table, loop_table):
    device_count = N_BLK * N_GRP
    slots = BLK_DEV + N_GRP + N_BLK
    fresh_blocks = features.astype(jnp.bfloat16).reshape(device_count, BLK_DEV, TILE, H)
    stale_blocks = history.reshape(device_count, BLK_DEV, TILE, H)
    start_blocks = initial.reshape(device_count, BLK_DEV, TILE, H)
    columns = column_ids.reshape(device_count, BLK_DEV, K)
    values = block_values.reshape(device_count, BLK_DEV, K, TILE, TILE)
    group_range = jnp.arange(N_GRP, dtype=jnp.int32)
    loop_range = jnp.arange(N_BLK, dtype=jnp.int32)
    slot_range = jnp.arange(slots, dtype=jnp.int32)

    def owners_of(device):
        loop_pos = device // N_GRP
        group_pos = device % N_GRP
        group_owner = loop_pos * N_GRP + group_range
        loop_owner = loop_range * N_GRP + group_pos
        group_block = group_table[loop_pos, :, group_pos]
        loop_block = loop_table[group_pos, :, loop_pos]
        owner = jnp.concatenate([group_owner, loop_owner]).astype(jnp.int32)
        block = jnp.concatenate([group_block, loop_block]).astype(jnp.int32)
        return owner, block

    def one_device(device):
        owner, block = owners_of(device)
        pulled = stale_blocks[owner, block]
        sources = jnp.concatenate([fresh_blocks[device], pulled], axis=0)
        column_rows = columns[device]
        picked = sources[column_rows].astype(jnp.float32)
        tile_values = values[device].astype(jnp.float32)
        gathered = jnp.einsum('tkij,tkjh->tih', tile_values, picked)
        start = start_blocks[device].astype(jnp.float32)
        mixed = ((1.0 - teleport) * gathered + teleport * start).astype(jnp.bfloat16).reshape(BLK_DEV * TILE, H)
        product = jnp.dot(mixed, weight, preferred_element_type=jnp.float32)
        refreshed = jax.nn.relu((1.0 - mapping_share) * mixed.astype(jnp.float32) + mapping_share * product)
        outgoing = refreshed.astype(jnp.bfloat16).reshape(BLK_DEV, TILE, H).astype(jnp.float32)
        each = jnp.einsum('tkij,tih->tkjh', tile_values, outgoing)
        selector = (column_rows[:, :, None] == slot_range[None, None, :]).astype(jnp.float32)
        messages = jnp.einsum('tks,tkjh->sjh', selector, each, precision=lax.Precision.HIGHEST)
        return refreshed, messages[BLK_DEV:].astype(jnp.bfloat16)

    device_ids = jnp.arange(device_count, dtype=jnp.int32)
    refreshed, messages = lax.map(one_device, device_ids)
    owner, block = jax.vmap(owners_of)(device_ids)
    targets = (owner * BLK_DEV + block).reshape(-1).astype(jnp.int32)
    inbox = jnp.zeros((device_count * BLK_DEV, TILE, H), jnp.float32)
    inbox = inbox.at[targets].add(messages.reshape(-1, TILE, H).astype(jnp.float32))
    return refreshed.reshape(NODES, H), inbox.reshape(NODES, H)
```

```python
import functools

import jax
import jax.numpy as jnp
from jax import lax
from jax.experimental import pallas as pl
from jax.experimental.pallas import tpu as pltpu
from jax.sharding import PartitionSpec as P

teleport = 0.1
mapping_share = 0.5
unroll = 8

ANY = pl.BlockSpec(memory_space=pl.ANY)
SMEM = pl.BlockSpec(memory_space=pltpu.SMEM)
VMEM = pl.BlockSpec(memory_space=pltpu.VMEM)


def shape(*dims, dtype=jnp.bfloat16):
    return jax.ShapeDtypeStruct(dims, dtype)


def pick_group_kernel(table, stale, out, sem):
    count = out.shape[0]
    mine = lax.axis_index("grp")
    copies = [pltpu.make_async_copy(stale.at[table[0, mine, r]], out.at[r], sem.at[r]) for r in range(count)]
    for copy in copies:
        copy.start()
    for copy in copies:
        copy.wait()


def pick_loop_kernel(table, stale, *refs):
    outs, sem = refs[:-1], refs[-1]
    count = len(outs)
    mine = lax.axis_index("blk")
    copies = [
        pltpu.make_async_copy(stale.at[table[0, mine, lax.rem(mine + o, count)]], out.at[0], sem.at[o])
        for o, out in enumerate(outs)
    ]
    for copy in copies:
        copy.start()
    for copy in copies:
        copy.wait()


def prepare_kernel(own_count, group_count, columns, features, own, entries, pair_slot, meta, count, place):
    own[...] = features[...].astype(jnp.bfloat16)
    tiles, width = columns.shape
    total = tiles * width
    slots = count.shape[0]
    loop_base = own_count + group_count
    room = pair_slot.shape[0]

    def clear(c, _):
        count[c] = 0
        return 0

    lax.fori_loop(0, slots, clear, 0)

    def tally(e, _):
        c = columns[e // width, e % width]
        count[c] = count[c] + 1
        return 0

    lax.fori_loop(0, total, tally, 0)

    def pairs_of(c, run):
        return run + (count[c] + 1) // 2

    group_pairs = lax.fori_loop(own_count, loop_base, pairs_of, 0)
    group_pairs = (group_pairs + unroll - 1) // unroll * unroll
    loop_pairs = lax.fori_loop(loop_base, slots, pairs_of, 0)
    loop_pairs = (loop_pairs + unroll - 1) // unroll * unroll
    meta[0] = group_pairs
    meta[1] = loop_pairs

    def blank(p, _):
        entries[2 * p] = total
        entries[2 * p + 1] = total
        pair_slot[p] = jnp.where(p < group_pairs, group_count, slots - loop_base)
        return 0

    lax.fori_loop(0, room, blank, 0)

    def lay_out(base):
        def step(c, run):
            place[c] = 2 * run
            size = (count[c] + 1) // 2

            def mark(i, _):
                pair_slot[run + i] = c - base
                return 0

            lax.fori_loop(0, size, mark, 0)
            return run + size

        return step

    lax.fori_loop(own_count, loop_base, lay_out(own_count), 0)
    lax.fori_loop(loop_base, slots, lay_out(loop_base), group_pairs)

    def enter(e, _):
        c = columns[e // width, e % width]

        @pl.when(c >= own_count)
        def _():
            at = place[c]
            entries[at] = e
            place[c] = at + 1

        return 0

    lax.fori_loop(0, total, enter, 0)


def add_messages(first, pairs, entries, pair_slot, turned, outgoing, total):
    tiles = outgoing.shape[0]
    width = (turned.shape[0] - 1) // tiles
    total[...] = jnp.zeros_like(total)

    def step(i, _):
        for u in range(unroll):
            p = first + i * unroll + u
            e0, e1 = entries[2 * p], entries[2 * p + 1]
            left = jnp.concatenate([turned[e0], turned[e1]], axis=1)
            t0, t1 = jnp.minimum(e0 // width, tiles - 1), jnp.minimum(e1 // width, tiles - 1)
            right = jnp.concatenate([outgoing[t0], outgoing[t1]], axis=0)
            slot = pair_slot[p]
            total[slot] = total[slot] + jnp.dot(left, right, preferred_element_type=jnp.float32)
        return 0

    lax.fori_loop(0, pairs // unroll, step, 0)


def layer_kernel(
    loop_count, columns, entries, pair_slot, meta, own, from_group, *refs
):
    from_loop = refs[:loop_count]
    (initial, weight, values, turned, refreshed, outgoing, messages) = refs[loop_count : loop_count + 7]
    (sources, start_v, weight_v, values_v, turned_v, mixed_v, refreshed_v, outgoing_v, total, message_v) = refs[
        loop_count + 7 : loop_count + 17
    ]
    sem, value_sem, turned_sem, out_sem = refs[loop_count + 17 :]
    tiles, edge, hidden = own.shape
    width = values.shape[1]
    group_count = from_group.shape[0]
    mine = lax.axis_index("blk")
    base = tiles + group_count

    copies = [
        pltpu.make_async_copy(own, sources.at[pl.ds(0, tiles)], sem.at[0]),
        pltpu.make_async_copy(initial, start_v, sem.at[1]),
        pltpu.make_async_copy(weight, weight_v, sem.at[2]),
    ]
    value_copies = [pltpu.make_async_copy(values.at[t], values_v.at[t], value_sem.at[t]) for t in range(tiles)]
    turned_copies = [
        pltpu.make_async_copy(
            turned.at[pl.ds(t * width, width)], turned_v.at[pl.ds(t * width, width)], turned_sem.at[t]
        )
        for t in range(tiles)
    ]
    for copy in copies + value_copies + turned_copies:
        copy.start()
    turned_v[tiles * width] = jnp.zeros((edge, edge), jnp.bfloat16)
    sources[pl.ds(tiles, group_count)] = from_group[...]
    for o in range(loop_count):
        sources[base + lax.rem(mine + loop_count - o, loop_count)] = from_loop[o][0]
    for copy in copies:
        copy.wait()

    for t in range(tiles):
        value_copies[t].wait()
        gathered = None
        for k in range(0, width, 2):
            left = jnp.concatenate([values_v[t, k], values_v[t, k + 1]], axis=1)
            right = jnp.concatenate([sources[columns[t, k]], sources[columns[t, k + 1]]], axis=0)
            part = jnp.dot(left, right, preferred_element_type=jnp.float32)
            gathered = part if gathered is None else gathered + part
        start = start_v[t].astype(jnp.float32)
        mixed_v[pl.ds(t * edge, edge)] = ((1.0 - teleport) * gathered + teleport * start).astype(jnp.bfloat16)

    for t in range(tiles):
        mixed = mixed_v[pl.ds(t * edge, edge)]
        product = jnp.dot(mixed, weight_v[...], preferred_element_type=jnp.float32)
        fresh = jax.nn.relu((1.0 - mapping_share) * mixed.astype(jnp.float32) + mapping_share * product)
        refreshed_v[t] = fresh
        outgoing_v[t] = fresh.astype(jnp.bfloat16)
    outs = [
        pltpu.make_async_copy(refreshed_v, refreshed, out_sem.at[0]),
        pltpu.make_async_copy(outgoing_v, outgoing, out_sem.at[1]),
    ]
    for copy in outs:
        copy.start()
    for copy in turned_copies:
        copy.wait()

    add_messages(0, meta[0], entries, pair_slot, turned_v, outgoing_v, total)
    half = group_count // 2
    for part in range(2):
        message_v[pl.ds(part * half, half)] = total[pl.ds(part * half, half)].astype(jnp.bfloat16)
        outs.append(
            pltpu.make_async_copy(
                message_v.at[pl.ds(part * half, half)], messages.at[pl.ds(part * half, half)], out_sem.at[2 + part]
            )
        )
        outs[-1].start()
    for copy in outs:
        copy.wait()


def loop_messages_kernel(loop_count, entries, pair_slot, meta, outgoing, turned, *refs):
    outs = refs[:loop_count]
    turned_v, total, message_v, sem, out_sem = refs[loop_count:]
    edge = turned.shape[1]
    count = turned.shape[0]
    mine = lax.axis_index("blk")
    copy = pltpu.make_async_copy(turned, turned_v.at[pl.ds(0, count)], sem.at[0])
    copy.start()
    turned_v[count] = jnp.zeros((edge, edge), jnp.bfloat16)
    copy.wait()
    add_messages(meta[0], meta[1], entries, pair_slot, turned_v, outgoing, total)
    message_v[...] = total[pl.ds(0, loop_count)].astype(jnp.bfloat16)
    copies = [
        pltpu.make_async_copy(message_v.at[lax.rem(mine + o, loop_count)], outs[o].at[0], out_sem.at[o])
        for o in range(loop_count)
    ]
    for c in copies:
        c.start()
    for c in copies:
        c.wait()


def inbox_kernel(loop_count, group_table, loop_table, from_group, *refs):
    from_loop = refs[:loop_count]
    inbox, total, out_sem = refs[loop_count:]
    group_count = from_group.shape[0]
    group_mine, loop_mine = lax.axis_index("grp"), lax.axis_index("blk")
    total[...] = jnp.zeros_like(total)
    for o in range(loop_count):
        reader = lax.rem(loop_mine + loop_count - o, loop_count)
        block = loop_table[0, loop_mine, reader]
        total[block] = total[block] + from_loop[o][0].astype(jnp.float32)
    for r in range(group_count):
        block = group_table[0, group_mine, r]
        total[block] = total[block] + from_group[r].astype(jnp.float32)
    out = pltpu.make_async_copy(total, inbox, out_sem)
    out.start()
    out.wait()


def near(x):
    return pltpu.with_memory_space_constraint(x, pltpu.VMEM)


def body(features, initial, history, weight, column_ids, block_values, group_table, loop_table):
    group_count = lax.axis_size("grp")
    loop_count = lax.axis_size("blk")
    tiles, width = column_ids.shape
    edge = block_values.shape[2]
    hidden = features.shape[1]
    slots = tiles + group_count + loop_count
    total = tiles * width
    room = (total + group_count + loop_count) // 2 + 3 * unroll
    block = (edge, hidden)
    stale = history.reshape(tiles, *block)
    dma = pltpu.SemaphoreType.DMA
    flops = 2 * total * edge * edge * hidden

    def around(block, shift):
        perm = [(i, (i + shift) % loop_count) for i in range(loop_count)]
        return block if shift == 0 else lax.ppermute(block, "blk", perm)

    to_group = pl.pallas_call(
        pick_group_kernel,
        out_shape=shape(group_count, *block),
        in_specs=[SMEM, VMEM],
        out_specs=ANY,
        scratch_shapes=[dma((group_count,))],
        name="pick_group",
    )(group_table, stale)
    from_group = lax.all_to_all(to_group, "grp", split_axis=0, concat_axis=0, tiled=True)

    to_loop = pl.pallas_call(
        pick_loop_kernel,
        out_shape=[shape(1, *block)] * loop_count,
        in_specs=[SMEM, VMEM],
        out_specs=[ANY] * loop_count,
        scratch_shapes=[dma((loop_count,))],
        name="pick_loop",
    )(loop_table, stale)
    from_loop = [around(to_loop[o], o) for o in range(loop_count)]

    turned = jnp.swapaxes(block_values, 2, 3).reshape(total, edge, edge)
    own, entries, pair_slot, meta = pl.pallas_call(
        functools.partial(prepare_kernel, tiles, group_count),
        out_shape=[
            shape(tiles, *block),
            shape(2 * room, dtype=jnp.int32),
            shape(room, dtype=jnp.int32),
            shape(2, dtype=jnp.int32),
        ],
        in_specs=[SMEM, VMEM],
        out_specs=[VMEM, SMEM, SMEM, SMEM],
        scratch_shapes=[pltpu.SMEM((slots,), jnp.int32), pltpu.SMEM((slots,), jnp.int32)],
        name="prepare",
    )(column_ids, features.reshape(tiles, *block))

    refreshed, outgoing, messages = pl.pallas_call(
        functools.partial(layer_kernel, loop_count),
        out_shape=[
            shape(tiles, *block, dtype=jnp.float32),
            shape(tiles, *block),
            shape(group_count, *block),
        ],
        in_specs=[SMEM] * 4 + [ANY] + [VMEM] * (loop_count + 1) + [ANY] * 4,
        out_specs=[ANY] * 3,
        scratch_shapes=[
            pltpu.VMEM((slots, *block), jnp.bfloat16),
            pltpu.VMEM((tiles, *block), jnp.bfloat16),
            pltpu.VMEM((hidden, hidden), jnp.bfloat16),
            pltpu.VMEM((tiles, width, edge, edge), jnp.bfloat16),
            pltpu.VMEM((total + 1, edge, edge), jnp.bfloat16),
            pltpu.VMEM((tiles * edge, hidden), jnp.bfloat16),
            pltpu.VMEM((tiles, *block), jnp.float32),
            pltpu.VMEM((tiles, *block), jnp.bfloat16),
            pltpu.VMEM((group_count + 1, *block), jnp.float32),
            pltpu.VMEM((group_count, *block), jnp.bfloat16),
            dma((3,)),
            dma((tiles,)),
            dma((tiles,)),
            dma((4,)),
        ],
        cost_estimate=pl.CostEstimate(flops=2 * flops, transcendentals=0, bytes_accessed=20 << 20),
        name="layer",
    )(
        column_ids,
        entries,
        pair_slot,
        meta,
        own,
        near(from_group),
        *from_loop,
        initial.reshape(tiles, *block),
        weight,
        block_values,
        turned,
    )
    incoming_group = lax.all_to_all(messages, "grp", split_axis=0, concat_axis=0, tiled=True)

    loop_messages = pl.pallas_call(
        functools.partial(loop_messages_kernel, loop_count),
        out_shape=[shape(1, *block)] * loop_count,
        in_specs=[SMEM] * 3 + [VMEM, ANY],
        out_specs=[ANY] * loop_count,
        scratch_shapes=[
            pltpu.VMEM((total + 1, edge, edge), jnp.bfloat16),
            pltpu.VMEM((loop_count + 1, *block), jnp.float32),
            pltpu.VMEM((loop_count, *block), jnp.bfloat16),
            dma((1,)),
            dma((loop_count,)),
        ],
        cost_estimate=pl.CostEstimate(flops=flops // 4, transcendentals=0, bytes_accessed=8 << 20),
        name="loop_messages",
    )(entries, pair_slot, meta, outgoing, turned)
    incoming_loop = [around(loop_messages[o], o) for o in range(loop_count)]

    inbox = pl.pallas_call(
        functools.partial(inbox_kernel, loop_count),
        out_shape=shape(tiles, *block, dtype=jnp.float32),
        in_specs=[SMEM] * 2 + [VMEM] * (loop_count + 1),
        out_specs=ANY,
        scratch_shapes=[pltpu.VMEM((tiles, *block), jnp.float32), dma],
        name="inbox",
    )(group_table, loop_table, near(incoming_group), *incoming_loop)
    return (refreshed.reshape(tiles * edge, hidden), inbox.reshape(tiles * edge, hidden))


def solution(mesh):
    in_specs = (
        P(("blk", "grp"), None),
        P(("blk", "grp"), None),
        P(("blk", "grp"), None),
        P(),
        P(("blk", "grp"), None),
        P(("blk", "grp"), None, None, None),
        P("blk", None, None),
        P("grp", None, None),
    )
    out_specs = (P(("blk", "grp"), None), P(("blk", "grp"), None))
    return jax.shard_map(body, mesh=mesh, in_specs=in_specs, out_specs=out_specs, check_vma=False)
```

```python
import functools

import jax
import jax.numpy as jnp
from jax import lax
from jax.experimental import pallas as pl
from jax.experimental.pallas import tpu as pltpu
from jax.sharding import PartitionSpec as P

teleport = 0.1
mapping_share = 0.5
lead = 4
unroll = 4

ANY = pl.BlockSpec(memory_space=pl.ANY)
SMEM = pl.BlockSpec(memory_space=pltpu.SMEM)
VMEM = pl.BlockSpec(memory_space=pltpu.VMEM)


def shape(*dims, dtype=jnp.bfloat16):
    return jax.ShapeDtypeStruct(dims, dtype)


def pick_group_kernel(table, stale, out, sem):
    mine = lax.axis_index("grp")
    copies = [
        pltpu.make_async_copy(stale.at[table[0, mine, r]], out.at[r], sem.at[r]) for r in range(out.shape[0])
    ]
    for copy in copies:
        copy.start()
    for copy in copies:
        copy.wait()


def pick_loop_kernel(table, stale, *refs):
    outs, sem = refs[:-1], refs[-1]
    count = len(outs)
    mine = lax.axis_index("blk")
    copies = [
        pltpu.make_async_copy(stale.at[table[0, mine, lax.rem(mine + o, count)]], out.at[0], sem.at[o])
        for o, out in enumerate(outs)
    ]
    for copy in copies:
        copy.start()
    for copy in copies:
        copy.wait()


def prepare_kernel(own_count, group_count, columns, features, own, first, rest, rest_slot, meta, count, place):
    own[...] = features[...].astype(jnp.bfloat16)
    tiles, width = columns.shape
    total = tiles * width
    slots = count.shape[0]
    loop_base = own_count + group_count
    room = rest_slot.shape[0]

    def clear(c, _):
        count[c] = 0
        return 0

    lax.fori_loop(0, slots, clear, 0)

    def tally(e, _):
        c = columns[e // width, e % width]
        count[c] = count[c] + 1
        return 0

    lax.fori_loop(0, total, tally, 0)

    def size(c):
        return jnp.maximum(count[c] - lead + 1, 0) // 2

    def pairs_of(c, run):
        return run + size(c)

    group_pairs = lax.fori_loop(own_count, loop_base, pairs_of, 0)
    group_pairs = (group_pairs + unroll - 1) // unroll * unroll
    loop_pairs = lax.fori_loop(loop_base, slots, pairs_of, 0)
    loop_pairs = (loop_pairs + unroll - 1) // unroll * unroll
    meta[0] = group_pairs
    meta[1] = loop_pairs

    def blank(p, _):
        rest[2 * p] = total
        rest[2 * p + 1] = total
        rest_slot[p] = 0
        return 0

    lax.fori_loop(0, group_pairs + loop_pairs, blank, 0)

    def blank_first(i, _):
        first[i] = total
        return 0

    lax.fori_loop(0, lead * (slots - own_count), blank_first, 0)

    def lay_out(base):
        def step(c, run):
            place[c] = 2 * run

            def mark(i, _):
                rest_slot[run + i] = c - base
                return 0

            lax.fori_loop(0, size(c), mark, 0)
            return run + size(c)

        return step

    lax.fori_loop(own_count, loop_base, lay_out(own_count), 0)
    lax.fori_loop(loop_base, slots, lay_out(loop_base), group_pairs)

    def restart(c, _):
        count[c] = 0
        return 0

    lax.fori_loop(0, slots, restart, 0)

    def enter(e, _):
        c = columns[e // width, e % width]
        seen = count[c]
        count[c] = seen + 1

        @pl.when((c >= own_count) & (seen < lead))
        def _():
            first[lead * (c - own_count) + seen] = e

        @pl.when((c >= own_count) & (seen >= lead))
        def _():
            rest[place[c] + seen - lead] = e

        return 0

    lax.fori_loop(0, total, enter, 0)


def product(listed, at, number, turned, outgoing):
    total = turned.shape[0]
    width = total // (outgoing.shape[0] - 1)
    chosen = [listed[at + i] for i in range(number)]
    left = jnp.concatenate([turned[jnp.minimum(e, total - 1)] for e in chosen], axis=1)
    right = jnp.concatenate([outgoing[e // width] for e in chosen], axis=0)
    return jnp.dot(left, right, preferred_element_type=jnp.float32)


def add_messages(slot_base, slots, pair_base, pairs, first, rest, rest_slot, turned, outgoing, total):
    for s in range(slots):
        total[s] = product(first, lead * (slot_base + s), lead, turned, outgoing)

    def step(i, _):
        for u in range(unroll):
            p = pair_base + i * unroll + u
            slot = rest_slot[p]
            total[slot] = total[slot] + product(rest, 2 * p, 2, turned, outgoing)
        return 0

    lax.fori_loop(0, pairs // unroll, step, 0)


def layer_kernel(loop_count, columns, first, rest, rest_slot, meta, own, from_group, *refs):
    from_loop = refs[:loop_count]
    initial, weight, values, turned, refreshed, outgoing, messages = refs[loop_count : loop_count + 7]
    (sources, start_v, weight_v, values_v, turned_v, mixed_v, refreshed_v, outgoing_v, total, message_v) = refs[
        loop_count + 7 : loop_count + 17
    ]
    sem, value_sem, turned_sem, out_sem = refs[loop_count + 17 :]
    tiles, edge, hidden = own.shape
    width = values.shape[1]
    group_count = from_group.shape[0]
    mine = lax.axis_index("blk")
    base = tiles + group_count

    source_copies = [pltpu.make_async_copy(own, sources.at[pl.ds(0, tiles)], sem.at[0])]
    for o in range(loop_count):
        owner = lax.rem(mine + loop_count - o, loop_count)
        source_copies.append(pltpu.make_async_copy(from_loop[o].at[0], sources.at[base + owner], sem.at[1 + o]))
    bounds = [0, 1, 4, 12]
    value_copies = [
        pltpu.make_async_copy(values.at[pl.ds(a, b - a)], values_v.at[pl.ds(a, b - a)], value_sem.at[i])
        for i, (a, b) in enumerate(zip(bounds, bounds[1:]))
    ]
    start_copy = pltpu.make_async_copy(initial, start_v, sem.at[loop_count + 1])
    weight_copy = pltpu.make_async_copy(weight, weight_v, sem.at[loop_count + 2])
    turned_copies = [pltpu.make_async_copy(turned, turned_v, turned_sem.at[0])]
    for copy in source_copies + value_copies[:1] + [start_copy] + value_copies[1:] + [weight_copy] + turned_copies:
        copy.start()
    sources[pl.ds(tiles, group_count)] = from_group[...]
    outgoing_v[tiles] = jnp.zeros((edge, hidden), jnp.bfloat16)
    for copy in source_copies:
        copy.wait()

    for t in range(tiles):
        if t in bounds:
            value_copies[bounds.index(t)].wait()
        left = jnp.concatenate([values_v[t, k] for k in range(width)], axis=1)
        right = jnp.concatenate([sources[columns[t, k]] for k in range(width)], axis=0)
        gathered = jnp.dot(left, right, preferred_element_type=jnp.float32)
        if t == 0:
            start_copy.wait()
        start = start_v[t].astype(jnp.float32)
        mixed_v[pl.ds(t * edge, edge)] = ((1.0 - teleport) * gathered + teleport * start).astype(jnp.bfloat16)

    weight_copy.wait()
    for t in range(tiles):
        mixed = mixed_v[pl.ds(t * edge, edge)]
        moved = jnp.dot(mixed, weight_v[...], preferred_element_type=jnp.float32)
        fresh = jax.nn.relu((1.0 - mapping_share) * mixed.astype(jnp.float32) + mapping_share * moved)
        refreshed_v[t] = fresh
        outgoing_v[t] = fresh.astype(jnp.bfloat16)
    outs = [
        pltpu.make_async_copy(refreshed_v, refreshed, out_sem.at[0]),
        pltpu.make_async_copy(outgoing_v, outgoing, out_sem.at[1]),
    ]
    for copy in outs:
        copy.start()
    for copy in turned_copies:
        copy.wait()

    add_messages(0, group_count, 0, meta[0], first, rest, rest_slot, turned_v, outgoing_v, total)
    parts = 4
    span = group_count // parts
    for part in range(parts):
        rows = pl.ds(part * span, span)
        message_v[rows] = total[rows].astype(jnp.bfloat16)
        outs.append(pltpu.make_async_copy(message_v.at[rows], messages.at[rows], out_sem.at[2 + part]))
        outs[-1].start()
    for copy in outs:
        copy.wait()


def loop_messages_kernel(loop_count, group_count, first, rest, rest_slot, meta, outgoing, turned, *refs):
    outs = refs[:loop_count]
    total, message_v, out_sem = refs[loop_count:]
    mine = lax.axis_index("blk")
    add_messages(group_count, loop_count, meta[0], meta[1], first, rest, rest_slot, turned, outgoing, total)
    message_v[...] = total[...].astype(jnp.bfloat16)
    copies = [
        pltpu.make_async_copy(message_v.at[lax.rem(mine + o, loop_count)], outs[o].at[0], out_sem.at[o])
        for o in range(loop_count)
    ]
    for c in copies:
        c.start()
    for c in copies:
        c.wait()


def inbox_kernel(loop_count, group_table, loop_table, from_group, *refs):
    from_loop = refs[:loop_count]
    inbox, total, out_sem = refs[loop_count:]
    group_count = from_group.shape[0]
    group_mine, loop_mine = lax.axis_index("grp"), lax.axis_index("blk")
    total[...] = jnp.zeros_like(total)
    for o in range(loop_count):
        reader = lax.rem(loop_mine + loop_count - o, loop_count)
        block = loop_table[0, loop_mine, reader]
        total[block] = total[block] + from_loop[o][0].astype(jnp.float32)
    for r in range(group_count):
        block = group_table[0, group_mine, r]
        total[block] = total[block] + from_group[r].astype(jnp.float32)
    out = pltpu.make_async_copy(total, inbox, out_sem)
    out.start()
    out.wait()


def near(x):
    return pltpu.with_memory_space_constraint(x, pltpu.VMEM)


def body(features, initial, history, weight, column_ids, block_values, group_table, loop_table):
    group_count = lax.axis_size("grp")
    loop_count = lax.axis_size("blk")
    tiles, width = column_ids.shape
    edge = block_values.shape[2]
    hidden = features.shape[1]
    slots = tiles + group_count + loop_count
    total = tiles * width
    room = (total + group_count + loop_count) // 2 + 3 * unroll
    block = (edge, hidden)
    stale = history.reshape(tiles, *block)
    dma = pltpu.SemaphoreType.DMA
    flops = 2 * total * edge * edge * hidden

    def around(block, shift):
        perm = [(i, (i + shift) % loop_count) for i in range(loop_count)]
        return block if shift == 0 else lax.ppermute(block, "blk", perm)

    to_group = pl.pallas_call(
        pick_group_kernel,
        out_shape=shape(group_count, *block),
        in_specs=[SMEM, VMEM],
        out_specs=ANY,
        scratch_shapes=[dma((group_count,))],
        name="pick_group",
    )(group_table, stale)
    from_group = lax.all_to_all(to_group, "grp", split_axis=0, concat_axis=0, tiled=True)

    to_loop = pl.pallas_call(
        pick_loop_kernel,
        out_shape=[shape(1, *block)] * loop_count,
        in_specs=[SMEM, VMEM],
        out_specs=[ANY] * loop_count,
        scratch_shapes=[dma((loop_count,))],
        name="pick_loop",
    )(loop_table, stale)
    from_loop = [around(to_loop[o], o) for o in range(loop_count)]

    turned = jnp.swapaxes(block_values, 2, 3).reshape(total, edge, edge)
    own, *lists = pl.pallas_call(
        functools.partial(prepare_kernel, tiles, group_count),
        out_shape=[
            shape(tiles, *block),
            shape(lead * (slots - tiles), dtype=jnp.int32),
            shape(2 * room, dtype=jnp.int32),
            shape(room, dtype=jnp.int32),
            shape(2, dtype=jnp.int32),
        ],
        in_specs=[SMEM, VMEM],
        out_specs=[VMEM] + [SMEM] * 4,
        scratch_shapes=[pltpu.SMEM((slots,), jnp.int32), pltpu.SMEM((slots,), jnp.int32)],
        name="prepare",
    )(column_ids, features.reshape(tiles, *block))

    refreshed, outgoing, messages = pl.pallas_call(
        functools.partial(layer_kernel, loop_count),
        out_shape=[
            shape(tiles, *block, dtype=jnp.float32),
            shape(tiles + 1, *block),
            shape(group_count, *block),
        ],
        in_specs=[SMEM] * 5 + [ANY, VMEM] + [ANY] * (loop_count + 4),
        out_specs=[ANY] * 3,
        scratch_shapes=[
            pltpu.VMEM((slots, *block), jnp.bfloat16),
            pltpu.VMEM((tiles, *block), jnp.bfloat16),
            pltpu.VMEM((hidden, hidden), jnp.bfloat16),
            pltpu.VMEM((tiles, width, edge, edge), jnp.bfloat16),
            pltpu.VMEM((total, edge, edge), jnp.bfloat16),
            pltpu.VMEM((tiles * edge, hidden), jnp.bfloat16),
            pltpu.VMEM((tiles, *block), jnp.float32),
            pltpu.VMEM((tiles + 1, *block), jnp.bfloat16),
            pltpu.VMEM((group_count, *block), jnp.float32),
            pltpu.VMEM((group_count, *block), jnp.bfloat16),
            dma((loop_count + 3,)),
            dma((tiles,)),
            dma((tiles,)),
            dma((6,)),
        ],
        cost_estimate=pl.CostEstimate(flops=2 * flops, transcendentals=0, bytes_accessed=20 << 20),
        name="layer",
    )(
        column_ids,
        *lists,
        own,
        near(from_group),
        *from_loop,
        initial.reshape(tiles, *block),
        weight,
        block_values,
        turned,
    )
    incoming_group = lax.all_to_all(messages, "grp", split_axis=0, concat_axis=0, tiled=True)

    loop_messages = pl.pallas_call(
        functools.partial(loop_messages_kernel, loop_count, group_count),
        out_shape=[shape(1, *block)] * loop_count,
        in_specs=[SMEM] * 4 + [VMEM] * 2,
        out_specs=[ANY] * loop_count,
        scratch_shapes=[
            pltpu.VMEM((loop_count, *block), jnp.float32),
            pltpu.VMEM((loop_count, *block), jnp.bfloat16),
            dma((loop_count,)),
        ],
        cost_estimate=pl.CostEstimate(flops=flops // 4, transcendentals=0, bytes_accessed=8 << 20),
        name="loop_messages",
    )(*lists, outgoing, turned)
    incoming_loop = [around(loop_messages[o], o) for o in range(loop_count)]

    inbox = pl.pallas_call(
        functools.partial(inbox_kernel, loop_count),
        out_shape=shape(tiles, *block, dtype=jnp.float32),
        in_specs=[SMEM] * 2 + [VMEM] * (loop_count + 1),
        out_specs=ANY,
        scratch_shapes=[pltpu.VMEM((tiles, *block), jnp.float32), dma],
        name="inbox",
    )(group_table, loop_table, near(incoming_group), *incoming_loop)
    return (refreshed.reshape(tiles * edge, hidden), inbox.reshape(tiles * edge, hidden))


def solution(mesh):
    in_specs = (
        P(("blk", "grp"), None),
        P(("blk", "grp"), None),
        P(("blk", "grp"), None),
        P(),
        P(("blk", "grp"), None),
        P(("blk", "grp"), None, None, None),
        P("blk", None, None),
        P("grp", None, None),
    )
    out_specs = (P(("blk", "grp"), None), P(("blk", "grp"), None))
    return jax.shard_map(body, mesh=mesh, in_specs=in_specs, out_specs=out_specs, check_vma=False)
```

```python
import functools

import jax
import jax.numpy as jnp
from jax import lax
from jax.experimental import pallas as pl
from jax.experimental.pallas import tpu as pltpu
from jax.sharding import PartitionSpec as P

teleport = 0.1
mapping_share = 0.5
lead = 6
unroll = 4

ANY = pl.BlockSpec(memory_space=pl.ANY)
SMEM = pl.BlockSpec(memory_space=pltpu.SMEM)
VMEM = pl.BlockSpec(memory_space=pltpu.VMEM)


def shape(*dims, dtype=jnp.bfloat16):
    return jax.ShapeDtypeStruct(dims, dtype)


def pick_group_kernel(table, stale, out, sem):
    mine = lax.axis_index("grp")
    copies = [
        pltpu.make_async_copy(stale.at[table[0, mine, r]], out.at[r], sem.at[r]) for r in range(out.shape[0])
    ]
    for copy in copies:
        copy.start()
    for copy in copies:
        copy.wait()


def pick_loop_kernel(table, stale, *refs):
    outs, sem = refs[:-1], refs[-1]
    count = len(outs)
    mine = lax.axis_index("blk")
    copies = [
        pltpu.make_async_copy(stale.at[table[0, mine, lax.rem(mine + o, count)]], out.at[0], sem.at[o])
        for o, out in enumerate(outs)
    ]
    for copy in copies:
        copy.start()
    for copy in copies:
        copy.wait()


def prepare_kernel(own_count, group_count, columns, features, own, first, rest, rest_slot, meta, count, place):
    own[...] = features[...].astype(jnp.bfloat16)
    tiles, width = columns.shape
    total = tiles * width
    slots = count.shape[0]
    loop_base = own_count + group_count
    room = rest_slot.shape[0]

    def clear(c, _):
        count[c] = 0
        return 0

    lax.fori_loop(0, slots, clear, 0)

    def tally(e, _):
        c = columns[e // width, e % width]
        count[c] = count[c] + 1
        return 0

    lax.fori_loop(0, total, tally, 0)

    def size(c):
        return jnp.maximum(count[c] - lead + 1, 0) // 2

    def pairs_of(c, run):
        return run + size(c)

    group_pairs = lax.fori_loop(own_count, loop_base, pairs_of, 0)
    group_pairs = (group_pairs + unroll - 1) // unroll * unroll
    loop_pairs = lax.fori_loop(loop_base, slots, pairs_of, 0)
    loop_pairs = (loop_pairs + unroll - 1) // unroll * unroll
    meta[0] = group_pairs
    meta[1] = loop_pairs

    def blank(p, _):
        rest[2 * p] = total
        rest[2 * p + 1] = total
        rest_slot[p] = 0
        return 0

    lax.fori_loop(0, group_pairs + loop_pairs, blank, 0)

    def blank_first(i, _):
        first[i] = total
        return 0

    lax.fori_loop(0, lead * (slots - own_count), blank_first, 0)

    def lay_out(base):
        def step(c, run):
            place[c] = 2 * run

            def mark(i, _):
                rest_slot[run + i] = c - base
                return 0

            lax.fori_loop(0, size(c), mark, 0)
            return run + size(c)

        return step

    lax.fori_loop(own_count, loop_base, lay_out(own_count), 0)
    lax.fori_loop(loop_base, slots, lay_out(loop_base), group_pairs)

    def restart(c, _):
        count[c] = 0
        return 0

    lax.fori_loop(0, slots, restart, 0)

    def enter(e, _):
        c = columns[e // width, e % width]
        seen = count[c]
        count[c] = seen + 1

        @pl.when((c >= own_count) & (seen < lead))
        def _():
            first[lead * (c - own_count) + seen] = e

        @pl.when((c >= own_count) & (seen >= lead))
        def _():
            rest[place[c] + seen - lead] = e

        return 0

    lax.fori_loop(0, total, enter, 0)


def product(listed, at, number, turned, outgoing):
    total = turned.shape[0]
    width = total // (outgoing.shape[0] - 1)
    chosen = [listed[at + i] for i in range(number)]
    left = jnp.concatenate([turned[jnp.minimum(e, total - 1)] for e in chosen], axis=1)
    right = jnp.concatenate([outgoing[e // width] for e in chosen], axis=0)
    return jnp.dot(left, right, preferred_element_type=jnp.float32)


def add_rest(pair_base, pairs, rest, rest_slot, turned, outgoing, total):
    def step(i, _):
        for u in range(unroll):
            p = pair_base + i * unroll + u
            slot = rest_slot[p]
            total[slot] = total[slot] + product(rest, 2 * p, 2, turned, outgoing)
        return 0

    lax.fori_loop(0, pairs // unroll, step, 0)


def layer_kernel(loop_count, columns, first, rest, rest_slot, meta, own, from_group, *refs):
    from_loop = refs[:loop_count]
    initial, weight, values, turned, refreshed, outgoing, messages = refs[loop_count : loop_count + 7]
    (sources, start_v, weight_v, values_v, turned_v, gathered_v, refreshed_v, outgoing_v, total, message_v) = refs[
        loop_count + 7 : loop_count + 17
    ]
    sem, value_sem, turned_sem, out_sem = refs[loop_count + 17 :]
    tiles, edge, hidden = own.shape
    width = values.shape[1]
    group_count = from_group.shape[0]
    mine = lax.axis_index("blk")
    base = tiles + group_count

    source_copies = [pltpu.make_async_copy(from_loop[0].at[0], sources.at[base + mine], sem.at[0])]
    bounds = [0, 1, 4, 12]
    value_copies = [
        pltpu.make_async_copy(values.at[pl.ds(a, b - a)], values_v.at[pl.ds(a, b - a)], value_sem.at[i])
        for i, (a, b) in enumerate(zip(bounds, bounds[1:]))
    ]
    start_copy = pltpu.make_async_copy(initial, start_v, sem.at[loop_count])
    weight_copy = pltpu.make_async_copy(weight, weight_v, sem.at[loop_count + 1])
    turned_copies = [pltpu.make_async_copy(turned, turned_v, turned_sem.at[0])]
    for copy in source_copies + value_copies + [start_copy, weight_copy] + turned_copies:
        copy.start()
    sources[pl.ds(0, tiles)] = own[...]
    sources[pl.ds(tiles, group_count)] = from_group[...]
    for o in range(1, loop_count):
        sources[base + lax.rem(mine + loop_count - o, loop_count)] = from_loop[o][0]
    total[...] = jnp.zeros_like(total)
    outgoing_v[tiles] = jnp.zeros((edge, hidden), jnp.bfloat16)
    for copy in source_copies:
        copy.wait()

    for t in range(tiles):
        if t in bounds:
            value_copies[bounds.index(t)].wait()
        left = jnp.concatenate([values_v[t, k] for k in range(width)], axis=1)
        right = jnp.concatenate([sources[columns[t, k]] for k in range(width)], axis=0)
        gathered = jnp.dot(left, right, preferred_element_type=jnp.float32)
        gathered_v[t] = gathered

    start_copy.wait()
    weight_copy.wait()
    for t in range(tiles):
        start = start_v[t].astype(jnp.float32)
        mixed = ((1.0 - teleport) * gathered_v[t] + teleport * start).astype(jnp.bfloat16)
        moved = jnp.dot(mixed, weight_v[...], preferred_element_type=jnp.float32)
        fresh = jax.nn.relu((1.0 - mapping_share) * mixed.astype(jnp.float32) + mapping_share * moved)
        refreshed_v[t] = fresh
        outgoing_v[t] = fresh.astype(jnp.bfloat16)
    outs = [
        pltpu.make_async_copy(refreshed_v, refreshed, out_sem.at[0]),
        pltpu.make_async_copy(outgoing_v, outgoing, out_sem.at[1]),
    ]
    for copy in outs:
        copy.start()
    for copy in turned_copies:
        copy.wait()

    add_rest(0, meta[0], rest, rest_slot, turned_v, outgoing_v, total)
    parts = out_sem.shape[0] - 2
    span = group_count // parts
    for part in range(parts):
        for c in range(part * span, part * span + span):
            message = product(first, lead * c, lead, turned_v, outgoing_v) + total[c]
            message_v[c] = message.astype(jnp.bfloat16)
        rows = pl.ds(part * span, span)
        outs.append(pltpu.make_async_copy(message_v.at[rows], messages.at[rows], out_sem.at[2 + part]))
        outs[-1].start()
    for copy in outs:
        copy.wait()


def loop_messages_kernel(loop_count, group_count, first, rest, rest_slot, meta, outgoing, turned, *refs):
    outs = refs[:loop_count]
    total, message_v, out_sem = refs[loop_count:]
    mine = lax.axis_index("blk")
    total[...] = jnp.zeros_like(total)
    add_rest(meta[0], meta[1], rest, rest_slot, turned, outgoing, total)
    for c in range(loop_count):
        message = product(first, lead * (group_count + c), lead, turned, outgoing) + total[c]
        message_v[c] = message.astype(jnp.bfloat16)
    copies = [
        pltpu.make_async_copy(message_v.at[lax.rem(mine + o, loop_count)], outs[o].at[0], out_sem.at[o])
        for o in range(loop_count)
    ]
    for c in copies:
        c.start()
    for c in copies:
        c.wait()


def inbox_kernel(loop_count, group_table, loop_table, from_group, *refs):
    from_loop = refs[:loop_count]
    inbox, total, out_sem = refs[loop_count:]
    group_count = from_group.shape[0]
    group_mine, loop_mine = lax.axis_index("grp"), lax.axis_index("blk")
    readers = [lax.rem(loop_mine + loop_count - o, loop_count) for o in range(loop_count)]
    loop_blocks = [loop_table[0, loop_mine, reader] for reader in readers]
    group_blocks = [group_table[0, group_mine, r] for r in range(group_count)]
    outs = []
    parts = out_sem.shape[0]
    span = total.shape[2] // parts
    for part in range(parts):
        columns = pl.ds(part * span, span)
        total[:, :, columns] = jnp.zeros((total.shape[0], total.shape[1], span), jnp.float32)
        for o in range(loop_count):
            block = loop_blocks[o]
            total[block, :, columns] = total[block, :, columns] + from_loop[o][0, :, columns].astype(jnp.float32)
        for r in range(group_count):
            block = group_blocks[r]
            total[block, :, columns] = total[block, :, columns] + from_group[r, :, columns].astype(jnp.float32)
        outs.append(pltpu.make_async_copy(total.at[:, :, columns], inbox.at[:, :, columns], out_sem.at[part]))
        outs[-1].start()
    for out in outs:
        out.wait()


def near(x):
    return pltpu.with_memory_space_constraint(x, pltpu.VMEM)


def body(features, initial, history, weight, column_ids, block_values, group_table, loop_table):
    group_count = lax.axis_size("grp")
    loop_count = lax.axis_size("blk")
    tiles, width = column_ids.shape
    edge = block_values.shape[2]
    hidden = features.shape[1]
    slots = tiles + group_count + loop_count
    total = tiles * width
    room = (total + group_count + loop_count) // 2 + 3 * unroll
    block = (edge, hidden)
    stale = history.reshape(tiles, *block)
    dma = pltpu.SemaphoreType.DMA
    flops = 2 * total * edge * edge * hidden

    def around(block, shift):
        perm = [(i, (i + shift) % loop_count) for i in range(loop_count)]
        return block if shift == 0 else lax.ppermute(block, "blk", perm)

    to_group = pl.pallas_call(
        pick_group_kernel,
        out_shape=shape(group_count, *block),
        in_specs=[SMEM, VMEM],
        out_specs=ANY,
        scratch_shapes=[dma((group_count,))],
        name="pick_group",
    )(group_table, stale)
    from_group = lax.all_to_all(to_group, "grp", split_axis=0, concat_axis=0, tiled=True)

    to_loop = pl.pallas_call(
        pick_loop_kernel,
        out_shape=[shape(1, *block)] * loop_count,
        in_specs=[SMEM, VMEM],
        out_specs=[ANY] * loop_count,
        scratch_shapes=[dma((loop_count,))],
        name="pick_loop",
    )(loop_table, stale)
    from_loop = [around(to_loop[o], o) for o in range(loop_count)]

    turned = jnp.swapaxes(block_values, 2, 3).reshape(total, edge, edge)
    own, *lists = pl.pallas_call(
        functools.partial(prepare_kernel, tiles, group_count),
        out_shape=[
            pltpu.VMEM((tiles, *block), jnp.bfloat16),
            shape(lead * (slots - tiles), dtype=jnp.int32),
            shape(2 * room, dtype=jnp.int32),
            shape(room, dtype=jnp.int32),
            shape(2, dtype=jnp.int32),
        ],
        in_specs=[SMEM, VMEM],
        out_specs=[VMEM] + [SMEM] * 4,
        scratch_shapes=[pltpu.SMEM((slots,), jnp.int32), pltpu.SMEM((slots,), jnp.int32)],
        name="prepare",
    )(column_ids, features.reshape(tiles, *block))

    refreshed, outgoing, messages = pl.pallas_call(
        functools.partial(layer_kernel, loop_count),
        out_shape=[
            shape(tiles, *block, dtype=jnp.float32),
            shape(tiles + 1, *block),
            shape(group_count, *block),
        ],
        in_specs=[SMEM] * 5 + [VMEM] * 2 + [ANY] + [VMEM] * (loop_count - 1) + [ANY] * 4,
        out_specs=[ANY] * 3,
        scratch_shapes=[
            pltpu.VMEM((slots, *block), jnp.bfloat16),
            pltpu.VMEM((tiles, *block), jnp.bfloat16),
            pltpu.VMEM((hidden, hidden), jnp.bfloat16),
            pltpu.VMEM((tiles, width, edge, edge), jnp.bfloat16),
            pltpu.VMEM((total, edge, edge), jnp.bfloat16),
            pltpu.VMEM((tiles, *block), jnp.float32),
            pltpu.VMEM((tiles, *block), jnp.float32),
            pltpu.VMEM((tiles + 1, *block), jnp.bfloat16),
            pltpu.VMEM((group_count, *block), jnp.float32),
            pltpu.VMEM((group_count, *block), jnp.bfloat16),
            dma((loop_count + 2,)),
            dma((tiles,)),
            dma((tiles,)),
            dma((10,)),
        ],
        cost_estimate=pl.CostEstimate(flops=2 * flops, transcendentals=0, bytes_accessed=20 << 20),
        name="layer",
    )(
        column_ids,
        *lists,
        near(own),
        near(from_group),
        from_loop[0],
        *[near(x) for x in from_loop[1:]],
        initial.reshape(tiles, *block),
        weight,
        block_values,
        turned,
    )
    incoming_group = lax.all_to_all(messages, "grp", split_axis=0, concat_axis=0, tiled=True)

    loop_messages = pl.pallas_call(
        functools.partial(loop_messages_kernel, loop_count, group_count),
        out_shape=[shape(1, *block)] * loop_count,
        in_specs=[SMEM] * 4 + [VMEM] * 2,
        out_specs=[ANY] * loop_count,
        scratch_shapes=[
            pltpu.VMEM((loop_count, *block), jnp.float32),
            pltpu.VMEM((loop_count, *block), jnp.bfloat16),
            dma((loop_count,)),
        ],
        cost_estimate=pl.CostEstimate(flops=flops // 4, transcendentals=0, bytes_accessed=8 << 20),
        name="loop_messages",
    )(*lists, outgoing, turned)
    incoming_loop = [around(loop_messages[o], o) for o in range(loop_count)]

    inbox = pl.pallas_call(
        functools.partial(inbox_kernel, loop_count),
        out_shape=shape(tiles, *block, dtype=jnp.float32),
        in_specs=[SMEM] * 2 + [VMEM] * (loop_count + 1),
        out_specs=ANY,
        scratch_shapes=[pltpu.VMEM((tiles, *block), jnp.float32), dma((2,))],
        name="inbox",
    )(group_table, loop_table, near(incoming_group), incoming_loop[0], *[near(x) for x in incoming_loop[1:]])
    return (refreshed.reshape(tiles * edge, hidden), inbox.reshape(tiles * edge, hidden))


def solution(mesh):
    in_specs = (
        P(("blk", "grp"), None),
        P(("blk", "grp"), None),
        P(("blk", "grp"), None),
        P(),
        P(("blk", "grp"), None),
        P(("blk", "grp"), None, None, None),
        P("blk", None, None),
        P("grp", None, None),
    )
    out_specs = (P(("blk", "grp"), None), P(("blk", "grp"), None))
    return jax.shard_map(body, mesh=mesh, in_specs=in_specs, out_specs=out_specs, check_vma=False)
```

```python
import functools

import jax
import jax.numpy as jnp
from jax import lax
from jax.experimental import pallas as pl
from jax.experimental.pallas import tpu as pltpu
from jax.sharding import PartitionSpec as P

teleport = 0.1
mapping_share = 0.5
lead = 6
unroll = 4

ANY = pl.BlockSpec(memory_space=pl.ANY)
SMEM = pl.BlockSpec(memory_space=pltpu.SMEM)
VMEM = pl.BlockSpec(memory_space=pltpu.VMEM)


def shape(*dims, dtype=jnp.bfloat16):
    return jax.ShapeDtypeStruct(dims, dtype)


def pick_group_kernel(table, stale, out, sem):
    mine = lax.axis_index("grp")
    copies = [
        pltpu.make_async_copy(stale.at[table[0, mine, r]], out.at[r], sem.at[r]) for r in range(out.shape[0])
    ]
    for copy in copies:
        copy.start()
    for copy in copies:
        copy.wait()


def pick_loop_kernel(table, stale, *refs):
    outs, sem = refs[:-1], refs[-1]
    count = len(outs)
    mine = lax.axis_index("blk")
    copies = [
        pltpu.make_async_copy(stale.at[table[0, mine, lax.rem(mine + o, count)]], out.at[0], sem.at[o])
        for o, out in enumerate(outs)
    ]
    for copy in copies:
        copy.start()
    for copy in copies:
        copy.wait()


def prepare_kernel(own_count, group_count, columns, features, own, first, rest, rest_slot, meta, count, place):
    own[...] = features[...].astype(jnp.bfloat16)
    tiles, width = columns.shape
    total = tiles * width
    slots = count.shape[0]
    loop_base = own_count + group_count
    room = rest_slot.shape[0]

    def clear(c, _):
        count[c] = 0
        return 0

    lax.fori_loop(0, slots, clear, 0)

    def tally(e, _):
        c = columns[e // width, e % width]
        count[c] = count[c] + 1
        return 0

    lax.fori_loop(0, total, tally, 0)

    def size(c):
        return jnp.maximum(count[c] - lead + 1, 0) // 2

    def pairs_of(c, run):
        return run + size(c)

    group_pairs = lax.fori_loop(own_count, loop_base, pairs_of, 0)
    group_pairs = (group_pairs + unroll - 1) // unroll * unroll
    loop_pairs = lax.fori_loop(loop_base, slots, pairs_of, 0)
    loop_pairs = (loop_pairs + unroll - 1) // unroll * unroll
    meta[0] = group_pairs
    meta[1] = loop_pairs

    def blank(p, _):
        rest[2 * p] = total
        rest[2 * p + 1] = total
        rest_slot[p] = 0
        return 0

    lax.fori_loop(0, group_pairs + loop_pairs, blank, 0)

    def blank_first(i, _):
        first[i] = total
        return 0

    lax.fori_loop(0, lead * (slots - own_count), blank_first, 0)

    def lay_out(base):
        def step(c, run):
            place[c] = 2 * run

            def mark(i, _):
                rest_slot[run + i] = c - base
                return 0

            lax.fori_loop(0, size(c), mark, 0)
            return run + size(c)

        return step

    lax.fori_loop(own_count, loop_base, lay_out(own_count), 0)
    lax.fori_loop(loop_base, slots, lay_out(loop_base), group_pairs)

    def restart(c, _):
        count[c] = 0
        return 0

    lax.fori_loop(0, slots, restart, 0)

    def enter(e, _):
        c = columns[e // width, e % width]
        seen = count[c]
        count[c] = seen + 1

        @pl.when((c >= own_count) & (seen < lead))
        def _():
            first[lead * (c - own_count) + seen] = e

        @pl.when((c >= own_count) & (seen >= lead))
        def _():
            rest[place[c] + seen - lead] = e

        return 0

    lax.fori_loop(0, total, enter, 0)


def product(listed, at, number, values, outgoing):
    total = values.shape[0]
    width = total // (outgoing.shape[0] - 1)
    chosen = [listed[at + i] for i in range(number)]
    left = jnp.concatenate([values[jnp.minimum(e, total - 1)] for e in chosen], axis=0)
    right = jnp.concatenate([outgoing[e // width] for e in chosen], axis=0)
    return lax.dot_general(left, right, (((0,), (0,)), ((), ())), preferred_element_type=jnp.float32)


def add_rest(pair_base, pairs, rest, rest_slot, values, outgoing, total):
    def step(i, _):
        for u in range(unroll):
            p = pair_base + i * unroll + u
            slot = rest_slot[p]
            total[slot] = total[slot] + product(rest, 2 * p, 2, values, outgoing)
        return 0

    lax.fori_loop(0, pairs // unroll, step, 0)


def layer_kernel(loop_count, columns, first, rest, rest_slot, meta, own, from_group, *refs):
    from_loop = refs[:loop_count]
    initial, weight, values, refreshed, outgoing, messages = refs[loop_count : loop_count + 6]
    (sources, start_v, weight_v, values_v, gathered_v, refreshed_v, outgoing_v, total, message_v) = refs[
        loop_count + 6 : loop_count + 15
    ]
    sem, value_sem, out_sem = refs[loop_count + 15 :]
    tiles, edge, hidden = own.shape
    width = values.shape[0] // tiles
    group_count = from_group.shape[0]
    mine = lax.axis_index("blk")
    base = tiles + group_count

    source_copies = [pltpu.make_async_copy(from_loop[0].at[0], sources.at[base + mine], sem.at[0])]
    bounds = [0, 2, 6, 12]
    value_copies = [
        pltpu.make_async_copy(
            values.at[pl.ds(a * width, (b - a) * width)], values_v.at[pl.ds(a * width, (b - a) * width)], value_sem.at[i]
        )
        for i, (a, b) in enumerate(zip(bounds, bounds[1:]))
    ]
    start_copy = pltpu.make_async_copy(initial, start_v, sem.at[loop_count])
    weight_copy = pltpu.make_async_copy(weight, weight_v, sem.at[loop_count + 1])
    for copy in source_copies + value_copies + [start_copy, weight_copy]:
        copy.start()
    sources[pl.ds(0, tiles)] = own[...]
    sources[pl.ds(tiles, group_count)] = from_group[...]
    for o in range(1, loop_count):
        sources[base + lax.rem(mine + loop_count - o, loop_count)] = from_loop[o][0]
    total[...] = jnp.zeros_like(total)
    outgoing_v[tiles] = jnp.zeros((edge, hidden), jnp.bfloat16)
    for copy in source_copies:
        copy.wait()

    for t in range(tiles):
        if t in bounds:
            value_copies[bounds.index(t)].wait()
        left = jnp.concatenate([values_v[t * width + k] for k in range(width)], axis=1)
        right = jnp.concatenate([sources[columns[t, k]] for k in range(width)], axis=0)
        gathered = jnp.dot(left, right, preferred_element_type=jnp.float32)
        gathered_v[t] = gathered

    start_copy.wait()
    weight_copy.wait()
    for t in range(tiles):
        start = start_v[t].astype(jnp.float32)
        mixed = ((1.0 - teleport) * gathered_v[t] + teleport * start).astype(jnp.bfloat16)
        moved = jnp.dot(mixed, weight_v[...], preferred_element_type=jnp.float32)
        fresh = jax.nn.relu((1.0 - mapping_share) * mixed.astype(jnp.float32) + mapping_share * moved)
        refreshed_v[t] = fresh
        outgoing_v[t] = fresh.astype(jnp.bfloat16)
    outs = [
        pltpu.make_async_copy(refreshed_v, refreshed, out_sem.at[0]),
        pltpu.make_async_copy(outgoing_v, outgoing, out_sem.at[1]),
    ]
    for copy in outs:
        copy.start()

    add_rest(0, meta[0], rest, rest_slot, values_v, outgoing_v, total)
    parts = out_sem.shape[0] - 2
    span = group_count // parts
    for part in range(parts):
        for c in range(part * span, part * span + span):
            message = product(first, lead * c, lead, values_v, outgoing_v) + total[c]
            message_v[c] = message.astype(jnp.bfloat16)
        rows = pl.ds(part * span, span)
        outs.append(pltpu.make_async_copy(message_v.at[rows], messages.at[rows], out_sem.at[2 + part]))
        outs[-1].start()
    for copy in outs:
        copy.wait()


def loop_messages_kernel(loop_count, group_count, first, rest, rest_slot, meta, outgoing, values, *refs):
    outs = refs[:loop_count]
    total, message_v, out_sem = refs[loop_count:]
    mine = lax.axis_index("blk")
    total[...] = jnp.zeros_like(total)
    add_rest(meta[0], meta[1], rest, rest_slot, values, outgoing, total)
    for c in range(loop_count):
        message = product(first, lead * (group_count + c), lead, values, outgoing) + total[c]
        message_v[c] = message.astype(jnp.bfloat16)
    copies = [
        pltpu.make_async_copy(message_v.at[lax.rem(mine + o, loop_count)], outs[o].at[0], out_sem.at[o])
        for o in range(loop_count)
    ]
    for c in copies:
        c.start()
    for c in copies:
        c.wait()


def inbox_kernel(loop_count, group_table, loop_table, from_group, *refs):
    from_loop = refs[:loop_count]
    inbox, total, out_sem = refs[loop_count:]
    group_count = from_group.shape[0]
    group_mine, loop_mine = lax.axis_index("grp"), lax.axis_index("blk")
    readers = [lax.rem(loop_mine + loop_count - o, loop_count) for o in range(loop_count)]
    loop_blocks = [loop_table[0, loop_mine, reader] for reader in readers]
    group_blocks = [group_table[0, group_mine, r] for r in range(group_count)]
    outs = []
    parts = out_sem.shape[0]
    span = total.shape[2] // parts
    for part in range(parts):
        columns = pl.ds(part * span, span)
        total[:, :, columns] = jnp.zeros((total.shape[0], total.shape[1], span), jnp.float32)
        for o in range(loop_count):
            block = loop_blocks[o]
            total[block, :, columns] = total[block, :, columns] + from_loop[o][0, :, columns].astype(jnp.float32)
        for r in range(group_count):
            block = group_blocks[r]
            total[block, :, columns] = total[block, :, columns] + from_group[r, :, columns].astype(jnp.float32)
        outs.append(pltpu.make_async_copy(total.at[:, :, columns], inbox.at[:, :, columns], out_sem.at[part]))
        outs[-1].start()
    for out in outs:
        out.wait()


def near(x):
    return pltpu.with_memory_space_constraint(x, pltpu.VMEM)


def body(features, initial, history, weight, column_ids, block_values, group_table, loop_table):
    group_count = lax.axis_size("grp")
    loop_count = lax.axis_size("blk")
    tiles, width = column_ids.shape
    edge = block_values.shape[2]
    hidden = features.shape[1]
    slots = tiles + group_count + loop_count
    total = tiles * width
    room = (total + group_count + loop_count) // 2 + 3 * unroll
    block = (edge, hidden)
    stale = history.reshape(tiles, *block)
    dma = pltpu.SemaphoreType.DMA
    flops = 2 * total * edge * edge * hidden

    def around(block, shift):
        perm = [(i, (i + shift) % loop_count) for i in range(loop_count)]
        return block if shift == 0 else lax.ppermute(block, "blk", perm)

    to_group = pl.pallas_call(
        pick_group_kernel,
        out_shape=shape(group_count, *block),
        in_specs=[SMEM, VMEM],
        out_specs=ANY,
        scratch_shapes=[dma((group_count,))],
        name="pick_group",
    )(group_table, stale)
    from_group = lax.all_to_all(to_group, "grp", split_axis=0, concat_axis=0, tiled=True)

    to_loop = pl.pallas_call(
        pick_loop_kernel,
        out_shape=[shape(1, *block)] * loop_count,
        in_specs=[SMEM, VMEM],
        out_specs=[ANY] * loop_count,
        scratch_shapes=[dma((loop_count,))],
        name="pick_loop",
    )(loop_table, stale)
    from_loop = [around(to_loop[o], o) for o in range(loop_count)]

    values = block_values.reshape(total, edge, edge)
    own, *lists = pl.pallas_call(
        functools.partial(prepare_kernel, tiles, group_count),
        out_shape=[
            pltpu.VMEM((tiles, *block), jnp.bfloat16),
            shape(lead * (slots - tiles), dtype=jnp.int32),
            shape(2 * room, dtype=jnp.int32),
            shape(room, dtype=jnp.int32),
            shape(2, dtype=jnp.int32),
        ],
        in_specs=[SMEM, VMEM],
        out_specs=[VMEM] + [SMEM] * 4,
        scratch_shapes=[pltpu.SMEM((slots,), jnp.int32), pltpu.SMEM((slots,), jnp.int32)],
        name="prepare",
    )(column_ids, features.reshape(tiles, *block))

    refreshed, outgoing, messages = pl.pallas_call(
        functools.partial(layer_kernel, loop_count),
        out_shape=[
            shape(tiles, *block, dtype=jnp.float32),
            shape(tiles + 1, *block),
            shape(group_count, *block),
        ],
        in_specs=[SMEM] * 5 + [VMEM] * 2 + [ANY] + [VMEM] * (loop_count - 1) + [ANY] * 3,
        out_specs=[ANY] * 3,
        scratch_shapes=[
            pltpu.VMEM((slots, *block), jnp.bfloat16),
            pltpu.VMEM((tiles, *block), jnp.bfloat16),
            pltpu.VMEM((hidden, hidden), jnp.bfloat16),
            pltpu.VMEM((total, edge, edge), jnp.bfloat16),
            pltpu.VMEM((tiles, *block), jnp.float32),
            pltpu.VMEM((tiles, *block), jnp.float32),
            pltpu.VMEM((tiles + 1, *block), jnp.bfloat16),
            pltpu.VMEM((group_count, *block), jnp.float32),
            pltpu.VMEM((group_count, *block), jnp.bfloat16),
            dma((loop_count + 2,)),
            dma((tiles,)),
            dma((10,)),
        ],
        cost_estimate=pl.CostEstimate(flops=2 * flops, transcendentals=0, bytes_accessed=20 << 20),
        name="layer",
    )(
        column_ids,
        *lists,
        near(own),
        near(from_group),
        from_loop[0],
        *[near(x) for x in from_loop[1:]],
        initial.reshape(tiles, *block),
        weight,
        values,
    )
    incoming_group = lax.all_to_all(messages, "grp", split_axis=0, concat_axis=0, tiled=True)

    loop_messages = pl.pallas_call(
        functools.partial(loop_messages_kernel, loop_count, group_count),
        out_shape=[shape(1, *block)] * loop_count,
        in_specs=[SMEM] * 4 + [VMEM] * 2,
        out_specs=[ANY] * loop_count,
        scratch_shapes=[
            pltpu.VMEM((loop_count, *block), jnp.float32),
            pltpu.VMEM((loop_count, *block), jnp.bfloat16),
            dma((loop_count,)),
        ],
        cost_estimate=pl.CostEstimate(flops=flops // 4, transcendentals=0, bytes_accessed=8 << 20),
        name="loop_messages",
    )(*lists, outgoing, values)
    incoming_loop = [around(loop_messages[o], o) for o in range(loop_count)]

    inbox = pl.pallas_call(
        functools.partial(inbox_kernel, loop_count),
        out_shape=shape(tiles, *block, dtype=jnp.float32),
        in_specs=[SMEM] * 2 + [VMEM] * (loop_count + 1),
        out_specs=ANY,
        scratch_shapes=[pltpu.VMEM((tiles, *block), jnp.float32), dma((2,))],
        name="inbox",
    )(group_table, loop_table, near(incoming_group), incoming_loop[0], *[near(x) for x in incoming_loop[1:]])
    return (refreshed.reshape(tiles * edge, hidden), inbox.reshape(tiles * edge, hidden))


def solution(mesh):
    in_specs = (
        P(("blk", "grp"), None),
        P(("blk", "grp"), None),
        P(("blk", "grp"), None),
        P(),
        P(("blk", "grp"), None),
        P(("blk", "grp"), None, None, None),
        P("blk", None, None),
        P("grp", None, None),
    )
    out_specs = (P(("blk", "grp"), None), P(("blk", "grp"), None))
    return jax.shard_map(body, mesh=mesh, in_specs=in_specs, out_specs=out_specs, check_vma=False)
```

```python
import functools

import jax
import jax.numpy as jnp
from jax import lax
from jax.experimental import pallas as pl
from jax.experimental.pallas import tpu as pltpu
from jax.sharding import PartitionSpec as P

teleport = 0.1
mapping_share = 0.5
lead = 6
unroll = 4

ANY = pl.BlockSpec(memory_space=pl.ANY)
SMEM = pl.BlockSpec(memory_space=pltpu.SMEM)
VMEM = pl.BlockSpec(memory_space=pltpu.VMEM)


def shape(*dims, dtype=jnp.bfloat16):
    return jax.ShapeDtypeStruct(dims, dtype)


def pick_group_kernel(table, stale, out, sem):
    mine = lax.axis_index("grp")
    copies = [
        pltpu.make_async_copy(stale.at[table[0, mine, r]], out.at[r], sem.at[r]) for r in range(out.shape[0])
    ]
    for copy in copies:
        copy.start()
    for copy in copies:
        copy.wait()


def pick_loop_kernel(table, stale, *refs):
    outs, sem = refs[:-1], refs[-1]
    count = len(outs)
    mine = lax.axis_index("blk")
    copies = [
        pltpu.make_async_copy(stale.at[table[0, mine, lax.rem(mine + o, count)]], out.at[0], sem.at[o])
        for o, out in enumerate(outs)
    ]
    for copy in copies:
        copy.start()
    for copy in copies:
        copy.wait()


def prepare_kernel(own_count, group_count, columns, features, own, first, rest, rest_slot, meta, count, place):
    own[...] = features[...].astype(jnp.bfloat16)
    tiles, width = columns.shape
    total = tiles * width
    slots = count.shape[0]
    loop_base = own_count + group_count
    room = rest_slot.shape[0]

    def clear(c, _):
        count[c] = 0
        return 0

    lax.fori_loop(0, slots, clear, 0)

    def tally(e, _):
        c = columns[e // width, e % width]
        count[c] = count[c] + 1
        return 0

    lax.fori_loop(0, total, tally, 0)

    def size(c):
        return jnp.maximum(count[c] - lead + 1, 0) // 2

    def pairs_of(c, run):
        return run + size(c)

    group_pairs = lax.fori_loop(own_count, loop_base, pairs_of, 0)
    group_pairs = (group_pairs + unroll - 1) // unroll * unroll
    loop_pairs = lax.fori_loop(loop_base, slots, pairs_of, 0)
    loop_pairs = (loop_pairs + unroll - 1) // unroll * unroll
    meta[0] = group_pairs
    meta[1] = loop_pairs

    def blank(p, _):
        rest[2 * p] = total
        rest[2 * p + 1] = total
        rest_slot[p] = 0
        return 0

    lax.fori_loop(0, group_pairs + loop_pairs, blank, 0)

    def blank_first(i, _):
        first[i] = total
        return 0

    lax.fori_loop(0, lead * (slots - own_count), blank_first, 0)

    def lay_out(base):
        def step(c, run):
            place[c] = 2 * run

            def mark(i, _):
                rest_slot[run + i] = c - base
                return 0

            lax.fori_loop(0, size(c), mark, 0)
            return run + size(c)

        return step

    lax.fori_loop(own_count, loop_base, lay_out(own_count), 0)
    lax.fori_loop(loop_base, slots, lay_out(loop_base), group_pairs)

    def restart(c, _):
        count[c] = 0
        return 0

    lax.fori_loop(0, slots, restart, 0)

    def enter(e, _):
        c = columns[e // width, e % width]
        seen = count[c]
        count[c] = seen + 1

        @pl.when((c >= own_count) & (seen < lead))
        def _():
            first[lead * (c - own_count) + seen] = e

        @pl.when((c >= own_count) & (seen >= lead))
        def _():
            rest[place[c] + seen - lead] = e

        return 0

    lax.fori_loop(0, total, enter, 0)


def product(listed, at, number, values, outgoing):
    total = values.shape[0]
    width = total // (outgoing.shape[0] - 1)
    chosen = [listed[at + i] for i in range(number)]
    left = jnp.concatenate([values[jnp.minimum(e, total - 1)] for e in chosen], axis=0)
    right = jnp.concatenate([outgoing[e // width] for e in chosen], axis=0)
    return lax.dot_general(left, right, (((0,), (0,)), ((), ())), preferred_element_type=jnp.float32)


def add_rest(pair_base, pairs, rest, rest_slot, values, outgoing, total):
    def step(i, _):
        for u in range(unroll):
            p = pair_base + i * unroll + u
            slot = rest_slot[p]
            total[slot] = total[slot] + product(rest, 2 * p, 2, values, outgoing)
        return 0

    lax.fori_loop(0, pairs // unroll, step, 0)


def layer_kernel(loop_count, columns, first, rest, rest_slot, meta, own, from_group, *refs):
    from_loop = refs[:loop_count]
    initial, weight, values, refreshed, outgoing, messages = refs[loop_count : loop_count + 6]
    (sources, start_v, weight_v, values_v, gathered_v, refreshed_v, outgoing_v, total, message_v) = refs[
        loop_count + 6 : loop_count + 15
    ]
    sem, value_sem, out_sem = refs[loop_count + 15 :]
    tiles, edge, hidden = own.shape
    width = values.shape[0] // tiles
    group_count = from_group.shape[0]
    mine = lax.axis_index("blk")
    base = tiles + group_count

    source_copies = [pltpu.make_async_copy(from_loop[0].at[0], sources.at[base + mine], sem.at[0])]
    bounds = [0, 2, 6, 12]
    value_copies = [
        pltpu.make_async_copy(
            values.at[pl.ds(a * width, (b - a) * width)], values_v.at[pl.ds(a * width, (b - a) * width)], value_sem.at[i]
        )
        for i, (a, b) in enumerate(zip(bounds, bounds[1:]))
    ]
    start_copy = pltpu.make_async_copy(initial, start_v, sem.at[loop_count])
    weight_copy = pltpu.make_async_copy(weight, weight_v, sem.at[loop_count + 1])
    for copy in source_copies + value_copies + [start_copy, weight_copy]:
        copy.start()
    sources[pl.ds(0, tiles)] = own[...]
    sources[pl.ds(tiles, group_count)] = from_group[...]
    for o in range(1, loop_count):
        sources[base + lax.rem(mine + loop_count - o, loop_count)] = from_loop[o][0]
    total[...] = jnp.zeros_like(total)
    outgoing_v[tiles] = jnp.zeros((edge, hidden), jnp.bfloat16)
    for copy in source_copies:
        copy.wait()

    for t in range(tiles):
        if t in bounds:
            value_copies[bounds.index(t)].wait()
        left = jnp.concatenate([values_v[t * width + k] for k in range(width)], axis=1)
        right = jnp.concatenate([sources[columns[t, k]] for k in range(width)], axis=0)
        gathered = jnp.dot(left, right, preferred_element_type=jnp.float32)
        gathered_v[t] = gathered

    start_copy.wait()
    weight_copy.wait()
    for t in range(tiles):
        start = start_v[t].astype(jnp.float32)
        mixed = ((1.0 - teleport) * gathered_v[t] + teleport * start).astype(jnp.bfloat16)
        moved = jnp.dot(mixed, weight_v[...], preferred_element_type=jnp.float32)
        fresh = jax.nn.relu((1.0 - mapping_share) * mixed.astype(jnp.float32) + mapping_share * moved)
        refreshed_v[t] = fresh
        outgoing_v[t] = fresh.astype(jnp.bfloat16)
    outs = [
        pltpu.make_async_copy(refreshed_v, refreshed, out_sem.at[0]),
        pltpu.make_async_copy(outgoing_v, outgoing, out_sem.at[1]),
    ]
    for copy in outs:
        copy.start()

    add_rest(0, meta[0], rest, rest_slot, values_v, outgoing_v, total)
    parts = out_sem.shape[0] - 2
    span = group_count // parts
    for part in range(parts):
        for c in range(part * span, part * span + span):
            message = product(first, lead * c, lead, values_v, outgoing_v) + total[c]
            message_v[c] = message.astype(jnp.bfloat16)
        rows = pl.ds(part * span, span)
        outs.append(pltpu.make_async_copy(message_v.at[rows], messages.at[rows], out_sem.at[2 + part]))
        outs[-1].start()
    for copy in outs:
        copy.wait()


def loop_messages_kernel(loop_count, group_count, first, rest, rest_slot, meta, outgoing, values, *refs):
    outs = refs[:loop_count]
    total, message_v, out_sem = refs[loop_count:]
    mine = lax.axis_index("blk")
    total[...] = jnp.zeros_like(total)
    add_rest(meta[0], meta[1], rest, rest_slot, values, outgoing, total)
    for c in range(loop_count):
        message = product(first, lead * (group_count + c), lead, values, outgoing) + total[c]
        message_v[c] = message.astype(jnp.bfloat16)
    copies = [
        pltpu.make_async_copy(message_v.at[lax.rem(mine + o, loop_count)], outs[o].at[0], out_sem.at[o])
        for o in range(loop_count)
    ]
    for c in copies:
        c.start()
    for c in copies:
        c.wait()


def inbox_kernel(loop_count, group_table, loop_table, from_group, *refs):
    from_loop = refs[:loop_count]
    inbox, total, out_sem = refs[loop_count:]
    group_count = from_group.shape[0]
    group_mine, loop_mine = lax.axis_index("grp"), lax.axis_index("blk")
    readers = [lax.rem(loop_mine + loop_count - o, loop_count) for o in range(loop_count)]
    loop_blocks = [loop_table[0, loop_mine, reader] for reader in readers]
    group_blocks = [group_table[0, group_mine, r] for r in range(group_count)]
    outs = []
    parts = out_sem.shape[0]
    span = total.shape[1] // parts
    for part in range(parts):
        rows = pl.ds(part * span, span)
        total[:, rows] = jnp.zeros((total.shape[0], span, total.shape[2]), jnp.float32)
        for o in range(loop_count):
            block = loop_blocks[o]
            total[block, rows] = total[block, rows] + from_loop[o][0, rows].astype(jnp.float32)
        for r in range(group_count):
            block = group_blocks[r]
            total[block, rows] = total[block, rows] + from_group[r, rows].astype(jnp.float32)
        outs.append(pltpu.make_async_copy(total.at[:, rows], inbox.at[:, rows], out_sem.at[part]))
        outs[-1].start()
    for out in outs:
        out.wait()


def near(x):
    return pltpu.with_memory_space_constraint(x, pltpu.VMEM)


def body(features, initial, history, weight, column_ids, block_values, group_table, loop_table):
    group_count = lax.axis_size("grp")
    loop_count = lax.axis_size("blk")
    tiles, width = column_ids.shape
    edge = block_values.shape[2]
    hidden = features.shape[1]
    slots = tiles + group_count + loop_count
    total = tiles * width
    room = (total + group_count + loop_count) // 2 + 3 * unroll
    block = (edge, hidden)
    stale = history.reshape(tiles, *block)
    dma = pltpu.SemaphoreType.DMA
    flops = 2 * total * edge * edge * hidden

    def around(block, shift):
        perm = [(i, (i + shift) % loop_count) for i in range(loop_count)]
        return block if shift == 0 else lax.ppermute(block, "blk", perm)

    to_group = pl.pallas_call(
        pick_group_kernel,
        out_shape=shape(group_count, *block),
        in_specs=[SMEM, VMEM],
        out_specs=ANY,
        scratch_shapes=[dma((group_count,))],
        name="pick_group",
    )(group_table, stale)
    from_group = lax.all_to_all(to_group, "grp", split_axis=0, concat_axis=0, tiled=True)

    to_loop = pl.pallas_call(
        pick_loop_kernel,
        out_shape=[shape(1, *block)] * loop_count,
        in_specs=[SMEM, VMEM],
        out_specs=[ANY] * loop_count,
        scratch_shapes=[dma((loop_count,))],
        name="pick_loop",
    )(loop_table, stale)
    from_loop = [around(to_loop[o], o) for o in range(loop_count)]

    values = block_values.reshape(total, edge, edge)
    own, *lists = pl.pallas_call(
        functools.partial(prepare_kernel, tiles, group_count),
        out_shape=[
            pltpu.VMEM((tiles, *block), jnp.bfloat16),
            shape(lead * (slots - tiles), dtype=jnp.int32),
            shape(2 * room, dtype=jnp.int32),
            shape(room, dtype=jnp.int32),
            shape(2, dtype=jnp.int32),
        ],
        in_specs=[SMEM, VMEM],
        out_specs=[VMEM] + [SMEM] * 4,
        scratch_shapes=[pltpu.SMEM((slots,), jnp.int32), pltpu.SMEM((slots,), jnp.int32)],
        name="prepare",
    )(column_ids, features.reshape(tiles, *block))

    refreshed, outgoing, messages = pl.pallas_call(
        functools.partial(layer_kernel, loop_count),
        out_shape=[
            shape(tiles, *block, dtype=jnp.float32),
            shape(tiles + 1, *block),
            shape(group_count, *block),
        ],
        in_specs=[SMEM] * 5 + [VMEM] * 2 + [ANY] + [VMEM] * (loop_count - 1) + [ANY] * 3,
        out_specs=[ANY] * 3,
        scratch_shapes=[
            pltpu.VMEM((slots, *block), jnp.bfloat16),
            pltpu.VMEM((tiles, *block), jnp.bfloat16),
            pltpu.VMEM((hidden, hidden), jnp.bfloat16),
            pltpu.VMEM((total, edge, edge), jnp.bfloat16),
            pltpu.VMEM((tiles, *block), jnp.float32),
            pltpu.VMEM((tiles, *block), jnp.float32),
            pltpu.VMEM((tiles + 1, *block), jnp.bfloat16),
            pltpu.VMEM((group_count, *block), jnp.float32),
            pltpu.VMEM((group_count, *block), jnp.bfloat16),
            dma((loop_count + 2,)),
            dma((tiles,)),
            dma((10,)),
        ],
        cost_estimate=pl.CostEstimate(flops=2 * flops, transcendentals=0, bytes_accessed=20 << 20),
        compiler_params=pltpu.CompilerParams(),
        name="layer",
    )(
        column_ids,
        *lists,
        near(own),
        near(from_group),
        from_loop[0],
        *[near(x) for x in from_loop[1:]],
        initial.reshape(tiles, *block),
        weight,
        values,
    )
    incoming_group = lax.all_to_all(messages, "grp", split_axis=0, concat_axis=0, tiled=True)

    loop_messages = pl.pallas_call(
        functools.partial(loop_messages_kernel, loop_count, group_count),
        out_shape=[shape(1, *block)] * loop_count,
        in_specs=[SMEM] * 4 + [VMEM] * 2,
        out_specs=[ANY] * loop_count,
        scratch_shapes=[
            pltpu.VMEM((loop_count, *block), jnp.float32),
            pltpu.VMEM((loop_count, *block), jnp.bfloat16),
            dma((loop_count,)),
        ],
        cost_estimate=pl.CostEstimate(flops=flops // 4, transcendentals=0, bytes_accessed=8 << 20),
        name="loop_messages",
    )(*lists, outgoing, values)
    incoming_loop = [around(loop_messages[o], o) for o in range(loop_count)]

    inbox = pl.pallas_call(
        functools.partial(inbox_kernel, loop_count),
        out_shape=shape(tiles, *block, dtype=jnp.float32),
        in_specs=[SMEM] * 2 + [VMEM] * (loop_count + 1),
        out_specs=ANY,
        scratch_shapes=[pltpu.VMEM((tiles, *block), jnp.float32), dma((4,))],
        name="inbox",
    )(group_table, loop_table, near(incoming_group), incoming_loop[0], *[near(x) for x in incoming_loop[1:]])
    return (refreshed.reshape(tiles * edge, hidden), inbox.reshape(tiles * edge, hidden))


def solution(mesh):
    in_specs = (
        P(("blk", "grp"), None),
        P(("blk", "grp"), None),
        P(("blk", "grp"), None),
        P(),
        P(("blk", "grp"), None),
        P(("blk", "grp"), None, None, None),
        P("blk", None, None),
        P("grp", None, None),
    )
    out_specs = (P(("blk", "grp"), None), P(("blk", "grp"), None))
    return jax.shard_map(body, mesh=mesh, in_specs=in_specs, out_specs=out_specs, check_vma=False)
```
